32 devices in a mesh: outer: 4 (over y, core), inner: 8 (over z, x).
Axes of the slice: x: 2, y: 2, z: 4, core: 2. Of those that a mesh axis runs over, the one named last changes fastest.
Arguments:
- amplitudes: float32 [2, 8388608], P(None, ('outer', 'inner')), may hold values from -200 to 200
Outputs:
- transformed: float32 [2, 8388608], P(None, ('outer', 'inner'))
- checks: float32 [3], replicated
The draws below stay inside these ranges and needn't reach their ends.
All inputs are finite; a program needn't handle non-finite values.
Results may differ from the reference program's by a relative error of at most 0.00007.
Values sent between devices are 32-bit elements; how exact they have to be, the bound alone decides.
A program may use at most 64 MiB of HBM per device.

```python
import math
import jax
import jax.numpy as jnp
from jax import lax

AMP_DEV = 262144
WINDOW = 9
DEVICES = 32


def draw_amplitudes(key, part):
    total_len = AMP_DEV * DEVICES
    first, second = jax.random.split(key, 2)
    position = jnp.arange(total_len, dtype=jnp.int32)
    device_pos = (position // AMP_DEV).astype(jnp.float32) / max(DEVICES - 1, 1)
    cell_scale = jnp.exp(jax.random.uniform(second, (total_len,), jnp.float32) * math.log(10.0))
    values = jnp.clip(jax.random.normal(first, (2, total_len), jnp.float32), -5.0, 5.0)
    ramp = 3.0 ** device_pos
    return values * ramp * cell_scale / 3.0


def setup_inputs(seed: int = 0) -> dict:
    streams_of = jax.random.split(jax.random.key(seed), 2)
    return {
        "amplitudes": draw_amplitudes(jax.random.fold_in(streams_of[1], 71), 0),
    }


def bit_reverse_table(count):
    result = []
    for value in range(2 ** count):
        flipped = 0
        for bit_pos in range(count):
            flipped = flipped | (value >> bit_pos & 1) << count - 1 - bit_pos
        result.append(flipped)
    return jnp.array(result, dtype=jnp.int32)

def reference(amplitudes):
    columns = 2 ** WINDOW
    total_len = AMP_DEV * DEVICES
    qubits = total_len.bit_length() - 1
    complex_amp = lax.complex(amplitudes[0], amplitudes[1]).reshape(-1, columns)
    spectrum = jnp.fft.ifft(complex_amp, axis=-1) * math.sqrt(columns)
    windowed = spectrum[:, bit_reverse_table(WINDOW)].reshape(-1)
    stacked = jnp.stack([jnp.real(windowed), jnp.imag(windowed)])
    expanded = stacked.reshape((2,) + (2,) * qubits)
    reversed_field = jnp.transpose(expanded, [0] + list(range(qubits, 0, -1))).reshape(2, total_len)
    mean_square = jnp.sum(reversed_field * reversed_field) / total_len
    factor = lax.rsqrt(mean_square + 1e-06)
    transformed = reversed_field * factor
    angles = jnp.arange(total_len, dtype=jnp.int32).astype(jnp.float32) * (2.0 * math.pi / total_len)
    cosine = jnp.cos(angles)
    sine = jnp.sin(angles)
    scaled = 1.0 / math.sqrt(total_len)
    phase_real = jnp.sum(transformed[0] * cosine + transformed[1] * sine) * scaled
    phase_imag = jnp.sum(transformed[1] * cosine - transformed[0] * sine) * scaled
    return (transformed, jnp.stack([mean_square, phase_real, phase_imag]))
```

```python
import functools
import math

import jax
import jax.numpy as jnp
import numpy as np
from jax import lax
from jax.experimental import pallas as pl
from jax.experimental.pallas import tpu as pltpu
from jax.sharding import PartitionSpec as P

WINDOW = 9
COLUMNS = 2**WINDOW
LANES = 128
SUB = 8
RADIX = COLUMNS // LANES
MESH = pl.DeviceIdType.MESH


def rev(value, count):
    out = 0
    for bit in range(count):
        out |= (value >> bit & 1) << (count - 1 - bit)
    return out


def split_bf16(values):
    high = values.astype(jnp.bfloat16)
    return high, (values - high.astype(np.float32)).astype(jnp.bfloat16)


def tables(rows_count, n_devices):
    f = np.arange(COLUMNS).reshape(LANES, RADIX).T
    lane = np.arange(LANES)
    ang = (f[:, :, None] * lane) % COLUMNS * (2.0 * np.pi / COLUMNS)
    c, s = np.cos(ang) / math.sqrt(COLUMNS), np.sin(ang) / math.sqrt(COLUMNS)
    table = np.stack([np.concatenate([c, -s], -1), np.concatenate([s, c], -1)], 2)
    table = table.reshape(RADIX, 2 * LANES, 2 * LANES).astype(np.float32)
    fa = f * (2.0 * np.pi / COLUMNS)
    cf = np.zeros((RADIX, SUB, LANES, 2), np.float32)
    cf[:, 0, :, 0], cf[:, 0, :, 1] = np.cos(fa), np.sin(fa)
    cf[:, 1, :, 0], cf[:, 1, :, 1] = -np.sin(fa), np.cos(fa)
    cf = cf.reshape(RADIX, SUB, 2 * LANES)
    bits = rows_count.bit_length() - 1
    ra = np.array([rev(r, bits) for r in range(rows_count)]) * (2.0 * np.pi / (rows_count * COLUMNS))
    cr = np.zeros((SUB, rows_count), np.float32)
    cr[0], cr[1] = np.cos(ra), np.sin(ra)
    return table, cf, cr


def swap_sublanes(v):
    at = lax.broadcasted_iota(jnp.int32, v.shape, 1)
    up, down = pltpu.roll(v, 5, 1), pltpu.roll(v, 3, 1)
    v = jnp.where((at == 1) | (at == 3), up, v)
    return jnp.where((at == 4) | (at == 6), down, v)


def kernel(n_outer, n_inner, rows_count, total_len, x_ref, th_ref, tl_ref, cf_ref, cr_ref, out_ref, tot_ref,
           sendbuf, recv, stat_out, stats, send_sem, recv_sem, own_sem, ssend_sem, srecv_sem):
    n_devices = n_outer * n_inner
    obits, ibits = n_outer.bit_length() - 1, n_inner.bit_length() - 1
    o, i = lax.axis_index("outer"), lax.axis_index("inner")
    me = o * n_inner + i
    slot = 0
    odelta, idelta = [], []
    for k in range(obits):
        bit = o // 2**k % 2
        slot = slot + bit * 2 ** (obits - 1 - k)
        odelta.append((1 - 2 * bit) * 2**k)
    for k in range(ibits):
        bit = i // 2**k % 2
        slot = slot + bit * 2 ** (ibits - 1 - k) * n_outer
        idelta.append((1 - 2 * bit) * 2**k)

    def peer(mo, mi):
        po, pi = o, i
        for k in range(obits):
            if mo >> k & 1:
                po = po + odelta[k]
        for k in range(ibits):
            if mi >> k & 1:
                pi = pi + idelta[k]
        return po, pi

    masks = [(mo, mi) for mi in reversed(range(n_inner)) for mo in reversed(range(n_outer)) if mo or mi]
    peers = [peer(mo, mi) for mo, mi in masks]

    barrier = pltpu.get_barrier_semaphore()
    for p in peers:
        pl.semaphore_signal(barrier, inc=1, device_id=p, device_id_type=MESH)

    groups = rows_count // LANES
    block = SUB * groups

    def data_copy(chunk, n):
        po, pi = peers[n]
        e = po * n_inner + pi
        return pltpu.make_async_remote_copy(
            src_ref=sendbuf.at[pl.ds(pl.multiple_of((chunk * n_devices + e) * block, block), block)],
            dst_ref=recv.at[pl.ds(pl.multiple_of((chunk * n_devices + slot) * block, block), block)],
            send_sem=send_sem.at[chunk, n], recv_sem=recv_sem.at[chunk, n],
            device_id=peers[n], device_id_type=MESH)

    def own_copy(chunk):
        return pltpu.make_async_copy(
            sendbuf.at[pl.ds(pl.multiple_of((chunk * n_devices + me) * block, block), block)],
            recv.at[pl.ds(pl.multiple_of((chunk * n_devices + slot) * block, block), block)],
            own_sem.at[chunk])

    def stat_copy(n):
        return pltpu.make_async_remote_copy(
            src_ref=stat_out, dst_ref=stats.at[slot],
            send_sem=ssend_sem.at[n], recv_sem=srecv_sem.at[n],
            device_id=peers[n], device_id_type=MESH)

    dims = (((1,), (1,)), ((), ()))
    parts = [[x_ref[pl.ds(2 * ct + s, rows_count, stride=2 * RADIX), :] for s in range(2)] for ct in range(RADIX)]
    (x0r, x0i), (x1r, x1i), (x2r, x2i), (x3r, x3i) = parts
    ar, ai, br, bi = x0r + x2r, x0i + x2i, x0r - x2r, x0i - x2i
    cr_, ci_, dr, di = x1r + x3r, x1i + x3i, x1r - x3r, x1i - x3i
    mixed = [(ar + cr_, ai + ci_), (br - di, bi + dr), (ar - cr_, ai - ci_), (br + di, bi - dr)]
    squares = jnp.zeros((SUB, LANES), jnp.float32)
    z = jnp.zeros((SUB, rows_count), jnp.float32)
    for chunk in range(RADIX):
        b = jnp.concatenate(mixed[chunk], 1)
        bh, bl = split_bf16(b)
        th, tl = th_ref[chunk], tl_ref[chunk]
        res = lax.dot_general(th, bh, dims, preferred_element_type=jnp.float32)
        res += lax.dot_general(th, bl, dims, preferred_element_type=jnp.float32)
        res += lax.dot_general(tl, bh, dims, preferred_element_type=jnp.float32)
        for e in range(n_devices):
            for g in range(groups):
                sendbuf[pl.ds(((chunk * n_devices + e) * groups + g) * SUB, SUB), :] = (
                    res[e * SUB:(e + 1) * SUB, g * LANES:(g + 1) * LANES])
        z += jnp.dot(cf_ref[chunk], res, precision=lax.Precision.HIGHEST, preferred_element_type=jnp.float32)
        sq = jnp.sum((res * res).reshape(-1, SUB, rows_count), 0)
        for g in range(groups):
            squares += sq[:, g * LANES:(g + 1) * LANES]
        if chunk == 0:
            pl.semaphore_wait(barrier, len(peers))
        if chunk == RADIX - 1:
            cosr, sinr, zr, zi = cr_ref[0:1, :], cr_ref[1:2, :], z[0:1, :], z[1:2, :]
            zre, zim = zr * cosr + zi * sinr, zi * cosr - zr * sinr
            fold = lambda v: sum(v[:, g * LANES:(g + 1) * LANES] for g in range(groups))
            stat_out[...] = jnp.concatenate(
                [jnp.sum(squares, 0, keepdims=True), fold(zre), fold(zim),
                 jnp.zeros((SUB - 3, LANES), jnp.float32)], 0)
            stats[pl.ds(slot, 1)] = stat_out[...][None]
            for n in range(len(peers)):
                stat_copy(n).start()
        for n in range(len(peers)):
            data_copy(chunk, n).start()
        own_copy(chunk).start()

    gbits = groups.bit_length() - 1
    for chunk in range(RADIX):
        for n in range(len(peers)):
            data_copy(chunk, n).wait_recv()
        own_copy(chunk).wait()
        for h in range(SUB):
            g = (h // 2) * RADIX + chunk
            tile = jnp.concatenate(
                [recv[pl.ds((chunk * n_devices * groups + rev(j, gbits)) * SUB + h, n_devices, stride=block), :]
                 for j in range(groups)], 0)
            turned = swap_sublanes(tile.T.reshape(LANES // SUB, SUB, LANES))
            for a in range(LANES // SUB):
                out_ref[pl.ds((g * LANES + rev(a, 4)) * 2 + h % 2, SUB, stride=2 * LANES // SUB), :] = turned[a]

    for n in range(len(peers)):
        stat_copy(n).wait_recv()
    t0 = t1 = t2 = jnp.zeros((SUB, LANES), jnp.float32)
    for q in range(n_devices):
        angle = 2.0 * math.pi * q / total_len
        v = stats[q]
        t0, t1, t2 = t0 + v, t1 + v * math.cos(angle), t2 + v * math.sin(angle)
    re = t1[1:2] + t2[2:3]
    im = t1[2:3] - t2[1:2]
    sums = jnp.concatenate([t0[0:1], re, im, jnp.zeros((SUB - 3, LANES), jnp.float32)], 0)
    tot_ref[...] = jnp.broadcast_to(jnp.sum(sums, 1, keepdims=True), (SUB, LANES))
    for n in range(len(peers)):
        stat_copy(n).wait_send()
        for chunk in range(RADIX):
            data_copy(chunk, n).wait_send()


def fast(n_outer, n_inner, amplitudes):
    amp_dev = amplitudes.shape[1]
    n_devices = n_outer * n_inner
    rows_count = amp_dev // COLUMNS
    total_len = amp_dev * n_devices
    view = amplitudes.reshape(2, amp_dev // LANES, LANES).transpose(1, 0, 2).reshape(-1, LANES)
    table, cf, cr = tables(rows_count, n_devices)
    th = table.astype(jnp.bfloat16)
    tl = (table - th.astype(np.float32)).astype(jnp.bfloat16)
    vmem = pl.BlockSpec(memory_space=pltpu.VMEM)
    n_peers = n_devices - 1
    field, tot = pl.pallas_call(
        functools.partial(kernel, n_outer, n_inner, rows_count, total_len),
        out_shape=(jax.ShapeDtypeStruct(view.shape, jnp.float32), jax.ShapeDtypeStruct((SUB, LANES), jnp.float32)),
        in_specs=[vmem] * 5,
        out_specs=(vmem, vmem),
        scratch_shapes=[
            pltpu.VMEM(view.shape, jnp.float32),
            pltpu.VMEM(view.shape, jnp.float32),
            pltpu.VMEM((SUB, LANES), jnp.float32),
            pltpu.VMEM((n_devices, SUB, LANES), jnp.float32),
            pltpu.SemaphoreType.DMA((RADIX, n_peers)),
            pltpu.SemaphoreType.DMA((RADIX, n_peers)),
            pltpu.SemaphoreType.DMA((RADIX,)),
            pltpu.SemaphoreType.DMA((n_peers,)),
            pltpu.SemaphoreType.DMA((n_peers,)),
        ],
        compiler_params=pltpu.CompilerParams(collective_id=0, has_side_effects=True,
                                             vmem_limit_bytes=32 * 2**20),
    )(view, jnp.asarray(th), jnp.asarray(tl), jnp.asarray(cf), jnp.asarray(cr))
    mean_square = tot[0, 0] / total_len
    factor = lax.rsqrt(mean_square + 1e-06)
    scaled = factor / math.sqrt(total_len)
    checks = jnp.stack([mean_square, tot[1, 0] * scaled, tot[2, 0] * scaled])
    result = (field * factor).reshape(-1, 2, LANES).transpose(1, 0, 2).reshape(2, amp_dev)
    return result, checks


def reverse_index(values, count):
    result = jnp.zeros_like(values)
    for bit_pos in range(count):
        result = result | (values >> bit_pos & 1) << count - 1 - bit_pos
    return result


def reversal_table(size, count):
    indices = jnp.arange(size, dtype=jnp.int32)
    return (reverse_index(indices, count)[:, None] == indices[None, :]).astype(jnp.float32)


def check_terms(current, positions, angle_scale):
    angles = positions.astype(jnp.float32) * angle_scale
    cosine = jnp.cos(angles)
    sine = jnp.sin(angles)
    squares = jnp.sum(current * current)
    phase_real = jnp.sum(current[0] * cosine + current[1] * sine)
    phase_imag = jnp.sum(current[1] * cosine - current[0] * sine)
    return (squares, phase_real, phase_imag)


def per_device(amplitudes):
    amp_dev = amplitudes.shape[1]
    n_outer = lax.axis_size("outer")
    n_inner = lax.axis_size("inner")
    outer_bits = n_outer.bit_length() - 1
    inner_bits = n_inner.bit_length() - 1
    global_bits = outer_bits + inner_bits
    local_bits = amp_dev.bit_length() - 1
    n_devices = n_outer * n_inner
    high_count = amp_dev // n_devices
    total_len = amp_dev * n_devices
    columns = 2**WINDOW
    rows_count = amp_dev // columns
    column_ids = jnp.arange(columns, dtype=jnp.int32)
    reversed_ids = reverse_index(column_ids, WINDOW)
    products = column_ids[:, None] * reversed_ids[None, :] % columns
    angles = products.astype(jnp.float32) * (2.0 * math.pi / columns)
    real_part = jnp.cos(angles) / math.sqrt(columns)
    imag_part = jnp.sin(angles) / math.sqrt(columns)
    table = jnp.concatenate(
        [jnp.concatenate([real_part, imag_part], 1), jnp.concatenate([-imag_part, real_part], 1)], 0
    )
    stacked = jnp.concatenate(
        [amplitudes[0].reshape(rows_count, columns), amplitudes[1].reshape(rows_count, columns)], 1
    )
    result = jnp.dot(
        stacked, table, precision=lax.Precision.HIGHEST, preferred_element_type=jnp.float32
    )
    windowed = jnp.stack([result[:, :columns].reshape(-1), result[:, columns:].reshape(-1)])
    device_id = lax.axis_index("outer") * n_inner + lax.axis_index("inner")
    angle_scale = 2.0 * math.pi / total_len
    local_ids = jnp.arange(amp_dev, dtype=jnp.int32)
    positions = reverse_index(device_id * amp_dev + local_ids, local_bits + global_bits)
    totals = lax.psum(check_terms(windowed, positions, angle_scale), ("outer", "inner"))
    device_table = reversal_table(n_devices, global_bits)
    high_table = reversal_table(high_count, local_bits - global_bits)
    grid = windowed.reshape(2, high_count, n_devices)
    ordered = jnp.einsum("pm,shm->sph", device_table, grid, precision=lax.Precision.HIGHEST)
    blocks = ordered.reshape(2, n_outer, n_inner, high_count)
    blocks = lax.all_to_all(
        lax.all_to_all(blocks, "outer", split_axis=1, concat_axis=1, tiled=True),
        "inner",
        split_axis=2,
        concat_axis=2,
        tiled=True,
    )
    received = blocks.reshape(2, n_devices, high_count)
    turned_high = jnp.einsum("qh,sdh->sdq", high_table, received, precision=lax.Precision.HIGHEST)
    placed = jnp.einsum("ed,sdq->sqe", device_table, turned_high, precision=lax.Precision.HIGHEST)
    reversed_field = placed.reshape(2, amp_dev)
    mean_square = totals[0] / total_len
    factor = lax.rsqrt(mean_square + 1e-06)
    scaled = factor / math.sqrt(total_len)
    checks = jnp.stack([mean_square, totals[1] * scaled, totals[2] * scaled])
    return (reversed_field * factor, checks)


def solution(mesh):
    n_outer, n_inner = mesh.shape["outer"], mesh.shape["inner"]

    def body(amplitudes):
        rows_count = amplitudes.shape[1] // COLUMNS
        n_devices = n_outer * n_inner
        if rows_count * n_devices == LANES * LANES and n_devices * SUB == 2 * LANES:
            return fast(n_outer, n_inner, amplitudes)
        return per_device(amplitudes)

    return jax.shard_map(
        body,
        mesh=mesh,
        in_specs=(P(None, ("outer", "inner")),),
        out_specs=(P(None, ("outer", "inner")), P()),
        check_vma=False,
    )
```

```python
import functools
import math

import jax
import jax.numpy as jnp
import numpy as np
from jax import lax
from jax.experimental import pallas as pl
from jax.experimental.pallas import tpu as pltpu
from jax.sharding import PartitionSpec as P

WINDOW = 9
COLUMNS = 2**WINDOW
LANES = 128
SUB = 8
RADIX = COLUMNS // LANES
MESH = pl.DeviceIdType.MESH


def rev(value, count):
    out = 0
    for bit in range(count):
        out |= (value >> bit & 1) << (count - 1 - bit)
    return out


def split_bf16(values):
    high = values.astype(jnp.bfloat16)
    return high, (values - high.astype(np.float32)).astype(jnp.bfloat16)


def tables(rows_count, n_devices):
    f = np.arange(COLUMNS).reshape(LANES, RADIX).T
    lane = np.arange(LANES)
    ang = (f[:, :, None] * lane) % COLUMNS * (2.0 * np.pi / COLUMNS)
    c, s = np.cos(ang) / math.sqrt(COLUMNS), np.sin(ang) / math.sqrt(COLUMNS)
    table = np.stack([np.concatenate([c, -s], -1), np.concatenate([s, c], -1)], 2)
    table = table.reshape(RADIX, 2 * LANES, 2 * LANES).astype(np.float32)
    fa = f * (2.0 * np.pi / COLUMNS)
    cf = np.zeros((RADIX, SUB, LANES, 2), np.float32)
    cf[:, 0, :, 0], cf[:, 0, :, 1] = np.cos(fa), np.sin(fa)
    cf[:, 1, :, 0], cf[:, 1, :, 1] = -np.sin(fa), np.cos(fa)
    cf = cf.reshape(RADIX, SUB, 2 * LANES)
    bits = rows_count.bit_length() - 1
    ra = np.array([rev(r, bits) for r in range(rows_count)]) * (2.0 * np.pi / (rows_count * COLUMNS))
    cr = np.zeros((SUB, rows_count), np.float32)
    cr[0], cr[1] = np.cos(ra), np.sin(ra)
    return table, cf, cr


def swap_sublanes(v):
    at = lax.broadcasted_iota(jnp.int32, v.shape, 1)
    up, down = pltpu.roll(v, 5, 1), pltpu.roll(v, 3, 1)
    v = jnp.where((at == 1) | (at == 3), up, v)
    return jnp.where((at == 4) | (at == 6), down, v)


def kernel(n_outer, n_inner, rows_count, total_len, x_hbm, th_hbm, tl_hbm, cf_hbm, cr_hbm, out_hbm, tot_ref, fac_ref,
           x_ref, th_ref, tl_ref, cf_ref, cr_ref, out_ref, sendbuf, recv, stat_out, stats, send_sem, recv_sem, own_sem, ssend_sem, srecv_sem, load_sem, out_sem):
    n_devices = n_outer * n_inner
    obits, ibits = n_outer.bit_length() - 1, n_inner.bit_length() - 1
    o, i = lax.axis_index("outer"), lax.axis_index("inner")
    me = o * n_inner + i
    slot = 0
    odelta, idelta = [], []
    for k in range(obits):
        bit = o // 2**k % 2
        slot = slot + bit * 2 ** (obits - 1 - k)
        odelta.append((1 - 2 * bit) * 2**k)
    for k in range(ibits):
        bit = i // 2**k % 2
        slot = slot + bit * 2 ** (ibits - 1 - k) * n_outer
        idelta.append((1 - 2 * bit) * 2**k)

    def peer(mo, mi):
        po, pi = o, i
        for k in range(obits):
            if mo >> k & 1:
                po = po + odelta[k]
        for k in range(ibits):
            if mi >> k & 1:
                pi = pi + idelta[k]
        return po, pi

    masks = [(mo, mi) for mi in range(n_inner) for mo in range(n_outer) if mo or mi]
    peers = [peer(mo, mi) for mo, mi in masks]

    barrier = pltpu.get_barrier_semaphore()
    for p in peers:
        pl.semaphore_signal(barrier, inc=1, device_id=p, device_id_type=MESH)

    loads = [pltpu.make_async_copy(src, dst, load_sem.at[k]) for k, (src, dst) in enumerate(
        [(x_hbm, x_ref), (th_hbm, th_ref), (tl_hbm, tl_ref), (cf_hbm, cf_ref), (cr_hbm, cr_ref)])]
    for load in loads:
        load.start()

    groups = rows_count // LANES
    block = SUB * groups

    def data_copy(chunk, n):
        po, pi = peers[n]
        e = po * n_inner + pi
        return pltpu.make_async_remote_copy(
            src_ref=sendbuf.at[pl.ds(pl.multiple_of((chunk * n_devices + e) * block, block), block)],
            dst_ref=recv.at[pl.ds(pl.multiple_of((chunk * n_devices + slot) * block, block), block)],
            send_sem=send_sem.at[chunk, n], recv_sem=recv_sem.at[chunk, n],
            device_id=peers[n], device_id_type=MESH)

    def own_copy(chunk):
        return pltpu.make_async_copy(
            sendbuf.at[pl.ds(pl.multiple_of((chunk * n_devices + me) * block, block), block)],
            recv.at[pl.ds(pl.multiple_of((chunk * n_devices + slot) * block, block), block)],
            own_sem.at[chunk])

    def stat_copy(n):
        return pltpu.make_async_remote_copy(
            src_ref=stat_out, dst_ref=stats.at[slot],
            send_sem=ssend_sem.at[n], recv_sem=srecv_sem.at[n],
            device_id=peers[n], device_id_type=MESH)

    def send(chunk):
        for n in range(len(peers)):
            data_copy(chunk, n).start()
        own_copy(chunk).start()

    dims = (((1,), (1,)), ((), ()))
    loads[0].wait()
    parts = [[x_ref[pl.ds(2 * ct + s, rows_count, stride=2 * RADIX), :] for s in range(2)] for ct in range(RADIX)]
    (x0r, x0i), (x1r, x1i), (x2r, x2i), (x3r, x3i) = parts
    ar, ai, br, bi = x0r + x2r, x0i + x2i, x0r - x2r, x0i - x2i
    cr_, ci_, dr, di = x1r + x3r, x1i + x3i, x1r - x3r, x1i - x3i
    mixed = [(ar + cr_, ai + ci_), (br - di, bi + dr), (ar - cr_, ai - ci_), (br + di, bi - dr)]
    squares = jnp.zeros((SUB, LANES), jnp.float32)
    z = jnp.zeros((SUB, rows_count), jnp.float32)
    for chunk in range(RADIX):
        b = jnp.concatenate(mixed[chunk], 1)
        bh, bl = split_bf16(b)
        if chunk == 0:
            for load in loads[1:]:
                load.wait()
        th, tl = th_ref[chunk], tl_ref[chunk]
        res = lax.dot_general(th, bh, dims, preferred_element_type=jnp.float32)
        res += lax.dot_general(th, bl, dims, preferred_element_type=jnp.float32)
        res += lax.dot_general(tl, bh, dims, preferred_element_type=jnp.float32)
        for e in range(n_devices):
            for g in range(groups):
                sendbuf[pl.ds(((chunk * n_devices + e) * groups + g) * SUB, SUB), :] = (
                    res[e * SUB:(e + 1) * SUB, g * LANES:(g + 1) * LANES])
        if chunk == 0:
            pl.semaphore_wait(barrier, len(peers))
        if chunk < RADIX - 1:
            send(chunk)
        z += jnp.dot(cf_ref[chunk], res, precision=lax.Precision.HIGHEST, preferred_element_type=jnp.float32)
        sq = jnp.sum((res * res).reshape(-1, SUB, rows_count), 0)
        for g in range(groups):
            squares += sq[:, g * LANES:(g + 1) * LANES]
        if chunk == RADIX - 1:
            cosr, sinr, zr, zi = cr_ref[0:1, :], cr_ref[1:2, :], z[0:1, :], z[1:2, :]
            zre, zim = zr * cosr + zi * sinr, zi * cosr - zr * sinr
            fold = lambda v: sum(v[:, g * LANES:(g + 1) * LANES] for g in range(groups))
            stat_out[...] = jnp.concatenate(
                [jnp.sum(squares, 0, keepdims=True), fold(zre), fold(zim),
                 jnp.zeros((SUB - 3, LANES), jnp.float32)], 0)
            stats[pl.ds(slot, 1)] = stat_out[...][None]
            for n in range(len(peers)):
                stat_copy(n).start()
            send(chunk)

    def out_copy(g):
        rows = pl.ds(g * 2 * LANES, 2 * LANES)
        return pltpu.make_async_copy(out_ref.at[rows], out_hbm.at[rows], out_sem.at[g])

    def finish_sums():
        for n in range(len(peers)):
            stat_copy(n).wait_recv()
        t0 = t1 = t2 = jnp.zeros((SUB, LANES), jnp.float32)
        for q in range(n_devices):
            angle = 2.0 * math.pi * q / total_len
            v = stats[q]
            t0, t1, t2 = t0 + v, t1 + v * math.cos(angle), t2 + v * math.sin(angle)
        re = t1[1:2] + t2[2:3]
        im = t1[2:3] - t2[1:2]
        sums = jnp.concatenate([t0[0:1], re, im, jnp.zeros((SUB - 3, LANES), jnp.float32)], 0)
        sums = jnp.sum(sums, 1, keepdims=True)
        mean_square = jnp.broadcast_to(sums[0:1], (SUB, LANES)) / total_len
        shifted = mean_square + 1e-06
        factor = lax.rsqrt(shifted)
        factor = factor * (1.5 - 0.5 * shifted * factor * factor)
        scaled = factor / math.sqrt(total_len)
        lane = lax.broadcasted_iota(jnp.int32, (SUB, LANES), 1)
        fac_ref[...] = factor
        tot_ref[...] = jnp.where(lane == 0, mean_square, jnp.where(lane == 1, sums[1:2], sums[2:3]) * scaled)

    gbits = groups.bit_length() - 1
    for chunk in range(RADIX):
        for n in range(len(peers)):
            data_copy(chunk, n).wait_recv()
        own_copy(chunk).wait()
        for h in range(SUB):
            g = (h // 2) * RADIX + chunk
            tile = jnp.concatenate(
                [recv[pl.ds((chunk * n_devices * groups + rev(j, gbits)) * SUB + h, n_devices, stride=block), :]
                 for j in range(groups)], 0)
            turned = swap_sublanes(tile.T.reshape(LANES // SUB, SUB, LANES))
            for a in range(LANES // SUB):
                out_ref[pl.ds((g * LANES + rev(a, 4)) * 2 + h % 2, SUB, stride=2 * LANES // SUB), :] = turned[a]
            if h % 2:
                out_copy(g).start()
        if chunk == RADIX - 2:
            finish_sums()
    for g in range(RADIX * SUB // 2):
        out_copy(g).wait()
    for n in range(len(peers)):
        stat_copy(n).wait_send()
        for chunk in range(RADIX):
            data_copy(chunk, n).wait_send()


def scale_kernel(field_ref, tot_ref, fac_ref, out_ref, checks_ref):
    field = field_ref[...]
    out_ref[...] = (field.reshape(-1, SUB, LANES) * fac_ref[...][None]).reshape(field.shape)
    checks_ref[...] = tot_ref[0:1, 0:3]


def fast(n_outer, n_inner, amplitudes):
    amp_dev = amplitudes.shape[1]
    n_devices = n_outer * n_inner
    rows_count = amp_dev // COLUMNS
    total_len = amp_dev * n_devices
    view = amplitudes.reshape(2, amp_dev // LANES, LANES).transpose(1, 0, 2).reshape(-1, LANES)
    table, cf, cr = tables(rows_count, n_devices)
    th = table.astype(jnp.bfloat16)
    tl = (table - th.astype(np.float32)).astype(jnp.bfloat16)
    vmem = pl.BlockSpec(memory_space=pltpu.VMEM)
    n_peers = n_devices - 1
    field, tot, fac = pl.pallas_call(
        functools.partial(kernel, n_outer, n_inner, rows_count, total_len),
        out_shape=(jax.ShapeDtypeStruct(view.shape, jnp.float32), *[jax.ShapeDtypeStruct((SUB, LANES), jnp.float32)] * 2),
        in_specs=[pl.BlockSpec(memory_space=pltpu.HBM)] * 5,
        out_specs=(pl.BlockSpec(memory_space=pltpu.HBM), vmem, vmem),
        scratch_shapes=[
            pltpu.VMEM(view.shape, jnp.float32),
            pltpu.VMEM(th.shape, jnp.bfloat16),
            pltpu.VMEM(tl.shape, jnp.bfloat16),
            pltpu.VMEM(cf.shape, jnp.float32),
            pltpu.VMEM(cr.shape, jnp.float32),
            pltpu.VMEM(view.shape, jnp.float32),
            pltpu.VMEM(view.shape, jnp.float32),
            pltpu.VMEM(view.shape, jnp.float32),
            pltpu.VMEM((SUB, LANES), jnp.float32),
            pltpu.VMEM((n_devices, SUB, LANES), jnp.float32),
            pltpu.SemaphoreType.DMA((RADIX, n_peers)),
            pltpu.SemaphoreType.DMA((RADIX, n_peers)),
            pltpu.SemaphoreType.DMA((RADIX,)),
            pltpu.SemaphoreType.DMA((n_peers,)),
            pltpu.SemaphoreType.DMA((n_peers,)),
            pltpu.SemaphoreType.DMA((5,)),
            pltpu.SemaphoreType.DMA((RADIX * SUB // 2,)),
        ],
        compiler_params=pltpu.CompilerParams(collective_id=0, has_side_effects=True,
                                             vmem_limit_bytes=63_500_000),
    )(view, jnp.asarray(th), jnp.asarray(tl), jnp.asarray(cf), jnp.asarray(cr))
    steps = 4
    rows = pl.BlockSpec((view.shape[0] // steps, LANES), lambda k: (k, 0))
    small = pl.BlockSpec((SUB, LANES), lambda k: (0, 0))
    field, checks = pl.pallas_call(
        scale_kernel,
        grid=(steps,),
        out_shape=(jax.ShapeDtypeStruct(view.shape, jnp.float32), jax.ShapeDtypeStruct((1, 3), jnp.float32)),
        in_specs=[rows, small, small],
        out_specs=(rows, pl.BlockSpec((1, 3), lambda k: (0, 0))),
        compiler_params=pltpu.CompilerParams(vmem_limit_bytes=63_500_000),
    )(field, tot, fac)
    result = field.reshape(-1, 2, LANES).transpose(1, 0, 2).reshape(2, amp_dev)
    return result, checks.reshape(3)


def reverse_index(values, count):
    result = jnp.zeros_like(values)
    for bit_pos in range(count):
        result = result | (values >> bit_pos & 1) << count - 1 - bit_pos
    return result


def reversal_table(size, count):
    indices = jnp.arange(size, dtype=jnp.int32)
    return (reverse_index(indices, count)[:, None] == indices[None, :]).astype(jnp.float32)


def check_terms(current, positions, angle_scale):
    angles = positions.astype(jnp.float32) * angle_scale
    cosine = jnp.cos(angles)
    sine = jnp.sin(angles)
    squares = jnp.sum(current * current)
    phase_real = jnp.sum(current[0] * cosine + current[1] * sine)
    phase_imag = jnp.sum(current[1] * cosine - current[0] * sine)
    return (squares, phase_real, phase_imag)


def per_device(amplitudes):
    amp_dev = amplitudes.shape[1]
    n_outer = lax.axis_size("outer")
    n_inner = lax.axis_size("inner")
    outer_bits = n_outer.bit_length() - 1
    inner_bits = n_inner.bit_length() - 1
    global_bits = outer_bits + inner_bits
    local_bits = amp_dev.bit_length() - 1
    n_devices = n_outer * n_inner
    high_count = amp_dev // n_devices
    total_len = amp_dev * n_devices
    columns = 2**WINDOW
    rows_count = amp_dev // columns
    column_ids = jnp.arange(columns, dtype=jnp.int32)
    reversed_ids = reverse_index(column_ids, WINDOW)
    products = column_ids[:, None] * reversed_ids[None, :] % columns
    angles = products.astype(jnp.float32) * (2.0 * math.pi / columns)
    real_part = jnp.cos(angles) / math.sqrt(columns)
    imag_part = jnp.sin(angles) / math.sqrt(columns)
    table = jnp.concatenate(
        [jnp.concatenate([real_part, imag_part], 1), jnp.concatenate([-imag_part, real_part], 1)], 0
    )
    stacked = jnp.concatenate(
        [amplitudes[0].reshape(rows_count, columns), amplitudes[1].reshape(rows_count, columns)], 1
    )
    result = jnp.dot(
        stacked, table, precision=lax.Precision.HIGHEST, preferred_element_type=jnp.float32
    )
    windowed = jnp.stack([result[:, :columns].reshape(-1), result[:, columns:].reshape(-1)])
    device_id = lax.axis_index("outer") * n_inner + lax.axis_index("inner")
    angle_scale = 2.0 * math.pi / total_len
    local_ids = jnp.arange(amp_dev, dtype=jnp.int32)
    positions = reverse_index(device_id * amp_dev + local_ids, local_bits + global_bits)
    totals = lax.psum(check_terms(windowed, positions, angle_scale), ("outer", "inner"))
    device_table = reversal_table(n_devices, global_bits)
    high_table = reversal_table(high_count, local_bits - global_bits)
    grid = windowed.reshape(2, high_count, n_devices)
    ordered = jnp.einsum("pm,shm->sph", device_table, grid, precision=lax.Precision.HIGHEST)
    blocks = ordered.reshape(2, n_outer, n_inner, high_count)
    blocks = lax.all_to_all(
        lax.all_to_all(blocks, "outer", split_axis=1, concat_axis=1, tiled=True),
        "inner",
        split_axis=2,
        concat_axis=2,
        tiled=True,
    )
    received = blocks.reshape(2, n_devices, high_count)
    turned_high = jnp.einsum("qh,sdh->sdq", high_table, received, precision=lax.Precision.HIGHEST)
    placed = jnp.einsum("ed,sdq->sqe", device_table, turned_high, precision=lax.Precision.HIGHEST)
    reversed_field = placed.reshape(2, amp_dev)
    mean_square = totals[0] / total_len
    factor = lax.rsqrt(mean_square + 1e-06)
    scaled = factor / math.sqrt(total_len)
    checks = jnp.stack([mean_square, totals[1] * scaled, totals[2] * scaled])
    return (reversed_field * factor, checks)


def solution(mesh):
    n_outer, n_inner = mesh.shape["outer"], mesh.shape["inner"]

    def body(amplitudes):
        rows_count = amplitudes.shape[1] // COLUMNS
        n_devices = n_outer * n_inner
        if rows_count * n_devices == LANES * LANES and n_devices * SUB == 2 * LANES:
            return fast(n_outer, n_inner, amplitudes)
        return per_device(amplitudes)

    return jax.shard_map(
        body,
        mesh=mesh,
        in_specs=(P(None, ("outer", "inner")),),
        out_specs=(P(None, ("outer", "inner")), P()),
        check_vma=False,
    )
```

```python
import functools
import math

import jax
import jax.numpy as jnp
import numpy as np
from jax import lax
from jax.experimental import pallas as pl
from jax.experimental.pallas import tpu as pltpu
from jax.sharding import PartitionSpec as P

WINDOW = 9
STEPS = 8
COLUMNS = 2**WINDOW
LANES = 128
SUB = 8
RADIX = COLUMNS // LANES
MESH = pl.DeviceIdType.MESH


def rev(value, count):
    out = 0
    for bit in range(count):
        out |= (value >> bit & 1) << (count - 1 - bit)
    return out


def split_bf16(values):
    high = values.astype(jnp.bfloat16)
    return high, (values - high.astype(np.float32)).astype(jnp.bfloat16)


def tables(rows_count, n_devices):
    f = np.arange(COLUMNS).reshape(LANES, RADIX).T
    lane = np.arange(LANES)
    ang = (f[:, :, None] * lane) % COLUMNS * (2.0 * np.pi / COLUMNS)
    c, s = np.cos(ang) / math.sqrt(COLUMNS), np.sin(ang) / math.sqrt(COLUMNS)
    table = np.stack([np.concatenate([c, -s], -1), np.concatenate([s, c], -1)], 2)
    table = table.reshape(RADIX, 2 * LANES, 2 * LANES).astype(np.float32)
    fa = f * (2.0 * np.pi / COLUMNS)
    cf = np.zeros((RADIX, SUB, LANES, 2), np.float32)
    cf[:, 0, :, 0], cf[:, 0, :, 1] = np.cos(fa), np.sin(fa)
    cf[:, 1, :, 0], cf[:, 1, :, 1] = -np.sin(fa), np.cos(fa)
    cf = cf.reshape(RADIX, SUB, 2 * LANES)
    bits = rows_count.bit_length() - 1
    ra = np.array([rev(r, bits) for r in range(rows_count)]) * (2.0 * np.pi / (rows_count * COLUMNS))
    cr = np.zeros((SUB, rows_count), np.float32)
    cr[0], cr[1] = np.cos(ra), np.sin(ra)
    return table, cf, cr


def swap_sublanes(v):
    at = lax.broadcasted_iota(jnp.int32, v.shape, 1)
    up, down = pltpu.roll(v, 5, 1), pltpu.roll(v, 3, 1)
    v = jnp.where((at == 1) | (at == 3), up, v)
    return jnp.where((at == 4) | (at == 6), down, v)


def kernel(n_outer, n_inner, rows_count, total_len, x_hbm, th_hbm, tl_hbm, cf_hbm, cr_hbm, out_hbm, tot_ref, fac_ref,
           x_ref, th_ref, tl_ref, cf_ref, cr_ref, out_ref, sendbuf, recv, stat_out, stats, send_sem, recv_sem, own_sem, ssend_sem, srecv_sem, load_sem, out_sem):
    n_devices = n_outer * n_inner
    obits, ibits = n_outer.bit_length() - 1, n_inner.bit_length() - 1
    o, i = lax.axis_index("outer"), lax.axis_index("inner")
    me = o * n_inner + i
    slot = 0
    odelta, idelta = [], []
    for k in range(obits):
        bit = o // 2**k % 2
        slot = slot + bit * 2 ** (obits - 1 - k)
        odelta.append((1 - 2 * bit) * 2**k)
    for k in range(ibits):
        bit = i // 2**k % 2
        slot = slot + bit * 2 ** (ibits - 1 - k) * n_outer
        idelta.append((1 - 2 * bit) * 2**k)

    def peer(mo, mi):
        po, pi = o, i
        for k in range(obits):
            if mo >> k & 1:
                po = po + odelta[k]
        for k in range(ibits):
            if mi >> k & 1:
                pi = pi + idelta[k]
        return po, pi

    masks = [(mo, mi) for mi in range(n_inner) for mo in range(n_outer) if mo or mi]
    peers = [peer(mo, mi) for mo, mi in masks]

    barrier = pltpu.get_barrier_semaphore()
    for p in peers:
        pl.semaphore_signal(barrier, inc=1, device_id=p, device_id_type=MESH)

    loads = [pltpu.make_async_copy(src, dst, load_sem.at[k]) for k, (src, dst) in enumerate(
        [(x_hbm, x_ref), (th_hbm, th_ref), (tl_hbm, tl_ref), (cf_hbm, cf_ref), (cr_hbm, cr_ref)])]
    for load in loads:
        load.start()

    groups = rows_count // LANES
    block = SUB * groups

    def data_copy(chunk, n):
        po, pi = peers[n]
        e = po * n_inner + pi
        return pltpu.make_async_remote_copy(
            src_ref=sendbuf.at[pl.ds(pl.multiple_of((chunk * n_devices + e) * block, block), block)],
            dst_ref=recv.at[pl.ds(pl.multiple_of((chunk * n_devices + slot) * block, block), block)],
            send_sem=send_sem.at[chunk, n], recv_sem=recv_sem.at[chunk, n],
            device_id=peers[n], device_id_type=MESH)

    def own_copy(chunk):
        return pltpu.make_async_copy(
            sendbuf.at[pl.ds(pl.multiple_of((chunk * n_devices + me) * block, block), block)],
            recv.at[pl.ds(pl.multiple_of((chunk * n_devices + slot) * block, block), block)],
            own_sem.at[chunk])

    def stat_copy(n):
        return pltpu.make_async_remote_copy(
            src_ref=stat_out, dst_ref=stats.at[slot],
            send_sem=ssend_sem.at[n], recv_sem=srecv_sem.at[n],
            device_id=peers[n], device_id_type=MESH)

    def send(chunk):
        for n in range(len(peers)):
            data_copy(chunk, n).start()
        own_copy(chunk).start()

    dims = (((1,), (1,)), ((), ()))
    loads[0].wait()
    parts = [[x_ref[pl.ds(2 * ct + s, rows_count, stride=2 * RADIX), :] for s in range(2)] for ct in range(RADIX)]
    (x0r, x0i), (x1r, x1i), (x2r, x2i), (x3r, x3i) = parts
    ar, ai, br, bi = x0r + x2r, x0i + x2i, x0r - x2r, x0i - x2i
    cr_, ci_, dr, di = x1r + x3r, x1i + x3i, x1r - x3r, x1i - x3i
    mixed = [(ar + cr_, ai + ci_), (br - di, bi + dr), (ar - cr_, ai - ci_), (br + di, bi - dr)]
    squares = jnp.zeros((SUB, LANES), jnp.float32)
    z = jnp.zeros((SUB, rows_count), jnp.float32)
    for chunk in range(RADIX):
        b = jnp.concatenate(mixed[chunk], 1)
        bh, bl = split_bf16(b)
        if chunk == 0:
            for load in loads[1:]:
                load.wait()
        th, tl = th_ref[chunk], tl_ref[chunk]
        res = lax.dot_general(th, bh, dims, preferred_element_type=jnp.float32)
        res += lax.dot_general(th, bl, dims, preferred_element_type=jnp.float32)
        res += lax.dot_general(tl, bh, dims, preferred_element_type=jnp.float32)
        for e in range(n_devices):
            for g in range(groups):
                sendbuf[pl.ds(((chunk * n_devices + e) * groups + g) * SUB, SUB), :] = (
                    res[e * SUB:(e + 1) * SUB, g * LANES:(g + 1) * LANES])
        if chunk == 0:
            pl.semaphore_wait(barrier, len(peers))
        if chunk < RADIX - 1:
            send(chunk)
        z += jnp.dot(cf_ref[chunk], res, precision=lax.Precision.HIGHEST, preferred_element_type=jnp.float32)
        sq = jnp.sum((res * res).reshape(-1, SUB, rows_count), 0)
        for g in range(groups):
            squares += sq[:, g * LANES:(g + 1) * LANES]
        if chunk == RADIX - 1:
            cosr, sinr, zr, zi = cr_ref[0:1, :], cr_ref[1:2, :], z[0:1, :], z[1:2, :]
            zre, zim = zr * cosr + zi * sinr, zi * cosr - zr * sinr
            fold = lambda v: sum(v[:, g * LANES:(g + 1) * LANES] for g in range(groups))
            stat_out[...] = jnp.concatenate(
                [jnp.sum(squares, 0, keepdims=True), fold(zre), fold(zim),
                 jnp.zeros((SUB - 3, LANES), jnp.float32)], 0)
            stats[pl.ds(slot, 1)] = stat_out[...][None]
            for n in range(len(peers)):
                stat_copy(n).start()
            send(chunk)

    def out_copy(g):
        rows = pl.ds(g * 2 * LANES, 2 * LANES)
        return pltpu.make_async_copy(out_ref.at[rows], out_hbm.at[rows], out_sem.at[g])

    def finish_sums():
        for n in range(len(peers)):
            stat_copy(n).wait_recv()
        t0 = t1 = t2 = jnp.zeros((SUB, LANES), jnp.float32)
        for q in range(n_devices):
            angle = 2.0 * math.pi * q / total_len
            v = stats[q]
            t0, t1, t2 = t0 + v, t1 + v * math.cos(angle), t2 + v * math.sin(angle)
        re = t1[1:2] + t2[2:3]
        im = t1[2:3] - t2[1:2]
        sums = jnp.concatenate([t0[0:1], re, im, jnp.zeros((SUB - 3, LANES), jnp.float32)], 0)
        sums = jnp.sum(sums, 1, keepdims=True)
        mean_square = jnp.broadcast_to(sums[0:1], (SUB, LANES)) / total_len
        shifted = mean_square + 1e-06
        factor = lax.rsqrt(shifted)
        factor = factor * (1.5 - 0.5 * shifted * factor * factor)
        scaled = factor / math.sqrt(total_len)
        lane = lax.broadcasted_iota(jnp.int32, (SUB, LANES), 1)
        fac_ref[...] = factor
        tot_ref[...] = jnp.where(lane == 0, mean_square, jnp.where(lane == 1, sums[1:2], sums[2:3]) * scaled)

    gbits = groups.bit_length() - 1
    for chunk in range(RADIX):
        for n in range(len(peers)):
            data_copy(chunk, n).wait_recv()
        own_copy(chunk).wait()
        for h in range(SUB):
            g = (h // 2) * RADIX + chunk
            tile = jnp.concatenate(
                [recv[pl.ds((chunk * n_devices * groups + rev(j, gbits)) * SUB + h, n_devices, stride=block), :]
                 for j in range(groups)], 0)
            turned = swap_sublanes(tile.T.reshape(LANES // SUB, SUB, LANES))
            for a in range(LANES // SUB):
                out_ref[pl.ds((g * LANES + rev(a, 4)) * 2 + h % 2, SUB, stride=2 * LANES // SUB), :] = turned[a]
            if h % 2:
                out_copy(g).start()
        if chunk == RADIX - 2:
            finish_sums()
    for g in range(RADIX * SUB // 2):
        out_copy(g).wait()
    for n in range(len(peers)):
        stat_copy(n).wait_send()
        for chunk in range(RADIX):
            data_copy(chunk, n).wait_send()


def scale_kernel(field_hbm, tot_ref, fac_ref, out_hbm, checks_ref, field, out, sem):
    size = field.shape[0] // STEPS
    pieces = [pl.ds(k * size, size) for k in range(STEPS)]
    loads = [pltpu.make_async_copy(field_hbm.at[p], field.at[p], sem.at[0, k]) for k, p in enumerate(pieces)]
    stores = [pltpu.make_async_copy(out.at[p], out_hbm.at[p], sem.at[1, k]) for k, p in enumerate(pieces)]
    for load in loads:
        load.start()
    checks_ref[...] = tot_ref[0:1, 0:3]
    for piece, load, store in zip(pieces, loads, stores):
        load.wait()
        out[piece, :] = (field[piece, :].reshape(-1, SUB, LANES) * fac_ref[...][None]).reshape(size, LANES)
        store.start()
    for store in stores:
        store.wait()


def fast(n_outer, n_inner, amplitudes):
    amp_dev = amplitudes.shape[1]
    n_devices = n_outer * n_inner
    rows_count = amp_dev // COLUMNS
    total_len = amp_dev * n_devices
    view = amplitudes.reshape(2, amp_dev // LANES, LANES).transpose(1, 0, 2).reshape(-1, LANES)
    table, cf, cr = tables(rows_count, n_devices)
    th = table.astype(jnp.bfloat16)
    tl = (table - th.astype(np.float32)).astype(jnp.bfloat16)
    vmem = pl.BlockSpec(memory_space=pltpu.VMEM)
    n_peers = n_devices - 1
    field, tot, fac = pl.pallas_call(
        functools.partial(kernel, n_outer, n_inner, rows_count, total_len),
        out_shape=(jax.ShapeDtypeStruct(view.shape, jnp.float32), *[jax.ShapeDtypeStruct((SUB, LANES), jnp.float32)] * 2),
        in_specs=[pl.BlockSpec(memory_space=pltpu.HBM)] * 5,
        out_specs=(pl.BlockSpec(memory_space=pltpu.HBM), vmem, vmem),
        scratch_shapes=[
            pltpu.VMEM(view.shape, jnp.float32),
            pltpu.VMEM(th.shape, jnp.bfloat16),
            pltpu.VMEM(tl.shape, jnp.bfloat16),
            pltpu.VMEM(cf.shape, jnp.float32),
            pltpu.VMEM(cr.shape, jnp.float32),
            pltpu.VMEM(view.shape, jnp.float32),
            pltpu.VMEM(view.shape, jnp.float32),
            pltpu.VMEM(view.shape, jnp.float32),
            pltpu.VMEM((SUB, LANES), jnp.float32),
            pltpu.VMEM((n_devices, SUB, LANES), jnp.float32),
            pltpu.SemaphoreType.DMA((RADIX, n_peers)),
            pltpu.SemaphoreType.DMA((RADIX, n_peers)),
            pltpu.SemaphoreType.DMA((RADIX,)),
            pltpu.SemaphoreType.DMA((n_peers,)),
            pltpu.SemaphoreType.DMA((n_peers,)),
            pltpu.SemaphoreType.DMA((5,)),
            pltpu.SemaphoreType.DMA((RADIX * SUB // 2,)),
        ],
        compiler_params=pltpu.CompilerParams(collective_id=0, has_side_effects=True,
                                             vmem_limit_bytes=63_500_000),
    )(view, jnp.asarray(th), jnp.asarray(tl), jnp.asarray(cf), jnp.asarray(cr))
    hbm = pl.BlockSpec(memory_space=pltpu.HBM)
    field, checks = pl.pallas_call(
        scale_kernel,
        out_shape=(jax.ShapeDtypeStruct(view.shape, jnp.float32), jax.ShapeDtypeStruct((1, 3), jnp.float32)),
        in_specs=[hbm, vmem, vmem],
        out_specs=(hbm, vmem),
        scratch_shapes=[
            pltpu.VMEM(view.shape, jnp.float32),
            pltpu.VMEM(view.shape, jnp.float32),
            pltpu.SemaphoreType.DMA((2, STEPS)),
        ],
        compiler_params=pltpu.CompilerParams(vmem_limit_bytes=63_500_000),
    )(field, tot, fac)
    result = field.reshape(-1, 2, LANES).transpose(1, 0, 2).reshape(2, amp_dev)
    return result, checks.reshape(3)


def reverse_index(values, count):
    result = jnp.zeros_like(values)
    for bit_pos in range(count):
        result = result | (values >> bit_pos & 1) << count - 1 - bit_pos
    return result


def reversal_table(size, count):
    indices = jnp.arange(size, dtype=jnp.int32)
    return (reverse_index(indices, count)[:, None] == indices[None, :]).astype(jnp.float32)


def check_terms(current, positions, angle_scale):
    angles = positions.astype(jnp.float32) * angle_scale
    cosine = jnp.cos(angles)
    sine = jnp.sin(angles)
    squares = jnp.sum(current * current)
    phase_real = jnp.sum(current[0] * cosine + current[1] * sine)
    phase_imag = jnp.sum(current[1] * cosine - current[0] * sine)
    return (squares, phase_real, phase_imag)


def per_device(amplitudes):
    amp_dev = amplitudes.shape[1]
    n_outer = lax.axis_size("outer")
    n_inner = lax.axis_size("inner")
    outer_bits = n_outer.bit_length() - 1
    inner_bits = n_inner.bit_length() - 1
    global_bits = outer_bits + inner_bits
    local_bits = amp_dev.bit_length() - 1
    n_devices = n_outer * n_inner
    high_count = amp_dev // n_devices
    total_len = amp_dev * n_devices
    columns = 2**WINDOW
    rows_count = amp_dev // columns
    column_ids = jnp.arange(columns, dtype=jnp.int32)
    reversed_ids = reverse_index(column_ids, WINDOW)
    products = column_ids[:, None] * reversed_ids[None, :] % columns
    angles = products.astype(jnp.float32) * (2.0 * math.pi / columns)
    real_part = jnp.cos(angles) / math.sqrt(columns)
    imag_part = jnp.sin(angles) / math.sqrt(columns)
    table = jnp.concatenate(
        [jnp.concatenate([real_part, imag_part], 1), jnp.concatenate([-imag_part, real_part], 1)], 0
    )
    stacked = jnp.concatenate(
        [amplitudes[0].reshape(rows_count, columns), amplitudes[1].reshape(rows_count, columns)], 1
    )
    result = jnp.dot(
        stacked, table, precision=lax.Precision.HIGHEST, preferred_element_type=jnp.float32
    )
    windowed = jnp.stack([result[:, :columns].reshape(-1), result[:, columns:].reshape(-1)])
    device_id = lax.axis_index("outer") * n_inner + lax.axis_index("inner")
    angle_scale = 2.0 * math.pi / total_len
    local_ids = jnp.arange(amp_dev, dtype=jnp.int32)
    positions = reverse_index(device_id * amp_dev + local_ids, local_bits + global_bits)
    totals = lax.psum(check_terms(windowed, positions, angle_scale), ("outer", "inner"))
    device_table = reversal_table(n_devices, global_bits)
    high_table = reversal_table(high_count, local_bits - global_bits)
    grid = windowed.reshape(2, high_count, n_devices)
    ordered = jnp.einsum("pm,shm->sph", device_table, grid, precision=lax.Precision.HIGHEST)
    blocks = ordered.reshape(2, n_outer, n_inner, high_count)
    blocks = lax.all_to_all(
        lax.all_to_all(blocks, "outer", split_axis=1, concat_axis=1, tiled=True),
        "inner",
        split_axis=2,
        concat_axis=2,
        tiled=True,
    )
    received = blocks.reshape(2, n_devices, high_count)
    turned_high = jnp.einsum("qh,sdh->sdq", high_table, received, precision=lax.Precision.HIGHEST)
    placed = jnp.einsum("ed,sdq->sqe", device_table, turned_high, precision=lax.Precision.HIGHEST)
    reversed_field = placed.reshape(2, amp_dev)
    mean_square = totals[0] / total_len
    factor = lax.rsqrt(mean_square + 1e-06)
    scaled = factor / math.sqrt(total_len)
    checks = jnp.stack([mean_square, totals[1] * scaled, totals[2] * scaled])
    return (reversed_field * factor, checks)


def solution(mesh):
    n_outer, n_inner = mesh.shape["outer"], mesh.shape["inner"]

    def body(amplitudes):
        rows_count = amplitudes.shape[1] // COLUMNS
        n_devices = n_outer * n_inner
        if rows_count * n_devices == LANES * LANES and n_devices * SUB == 2 * LANES:
            return fast(n_outer, n_inner, amplitudes)
        return per_device(amplitudes)

    return jax.shard_map(
        body,
        mesh=mesh,
        in_specs=(P(None, ("outer", "inner")),),
        out_specs=(P(None, ("outer", "inner")), P()),
        check_vma=False,
    )
```
